32 devices in a mesh: rep: 2 (over x), blk: 16 (over z, y, core).
Axes of the slice: x: 2, y: 2, z: 4, core: 2. Of those that a mesh axis runs over, the one named last changes fastest.
Arguments:
- hidden: bfloat16 [32, 4096], P('rep', 'blk'), parts along dimension 0, may hold values from -4 to 4
- queries: bfloat16 [32, 4096], P('rep'), parts along dimension 0, may hold values from -180 to 180
- cache_kv: bfloat16 [2, 32, 512, 1024], P(None, 'rep', 'blk'), parts along dimension 1, may hold values from -6 to 6
- cache_len: int32 [32], P('rep'), parts along dimension 0, may hold values from 1 to 512
- inserted_key_value: bfloat16 [2, 16, 512, 1024], P(None, 'rep', 'blk'), parts along dimension 1, may hold values from -6 to 6
- insert_slot: int32 [16], P('rep'), parts along dimension 0, may hold values from 0 to 15, as said below
- prefix_len: int32 [16], P('rep'), parts along dimension 0, may hold values from 1 to 512, as said below
- out_weight: bfloat16 [4096, 4096], P(None, 'blk'), may hold values from -0.09375 to 0.09375
- norm_gain: bfloat16 [4096], replicated, may hold values from 0.25 to 1.75
- router_weight: bfloat16 [4096, 4], replicated, may hold values from -0.09375 to 0.09375
- expert_ids: int32 [32, 2], P('rep'), parts along dimension 0, may hold values from 0 to 3, all different within a row
- gate_up: bfloat16 [2, 4096, 28672], P(None, None, 'blk'), may hold values from -0.09375 to 0.09375
- down_proj: bfloat16 [28672, 4096], P('blk'), may hold values from -0.0625 to 0.0625
Outputs:
- layer_out: bfloat16 [32, 4096], P('rep', 'blk'), parts along dimension 0
The draws below stay inside these ranges and needn't reach their ends.
There are 2 independent parts, one for each index of `rep`. The reference program is written for one: setup_inputs(seed, part) draws one part's arguments, and reference() takes and returns one part's arrays. A program takes and returns all parts, laid end to end along the dimension named above; an argument that names none is the same for every part. Nothing has to cross between parts.
Inputs may be any that keep to these rules, and one draw needn't show every extreme that they name: `insert_slot`: 8 different slot numbers. `prefix_len`: some inserted request has all 512 positions.
All inputs are finite; a program needn't handle non-finite values.
Results may differ from the reference program's by a relative error of at most 0.012.
Values may be sent and summed in bfloat16 or wider, within the bound.
A program may use at most 128 MiB of HBM per device.

```python
import math
import jax
import jax.numpy as jnp
from jax import lax

D = 4096
QUERY_HEADS = 32
KEY_VALUE_HEADS = 8
HEAD_SIZE = 128
EXPERTS = 4
FF = 7168
SLOTS = 16
INSERTED_SLOTS = 8
CACHE_POSITIONS = 512


def slot_order(key):
    return jax.random.permutation(jax.random.fold_in(key, 11), SLOTS).astype(jnp.int32)


def cache_lengths(key):
    return jax.random.randint(jax.random.fold_in(key, 12), (SLOTS,), 1, CACHE_POSITIONS + 1).astype(jnp.int32)


def rows_per_slot(key, slot_entry):
    cache_rows = jax.random.normal(jax.random.fold_in(jax.random.fold_in(key, 13), slot_entry), (2, CACHE_POSITIONS, KEY_VALUE_HEADS * HEAD_SIZE), jnp.float32)
    return jnp.clip(cache_rows, -6.0, 6.0)


def inserted_rows(key):
    drawn = jax.random.normal(jax.random.fold_in(key, 41), (2, INSERTED_SLOTS, CACHE_POSITIONS, KEY_VALUE_HEADS * HEAD_SIZE), jnp.float32)
    return jnp.clip(drawn, -6.0, 6.0)


def longest_request(key):
    return jax.random.randint(jax.random.fold_in(key, 32), (), 0, INSERTED_SLOTS).astype(jnp.int32)


def draw_insert_slot(key, part):
    return slot_order(key)[:INSERTED_SLOTS]


def draw_prefix_len(key, part):
    drawn = jax.random.randint(jax.random.fold_in(key, 31), (INSERTED_SLOTS,), 1, CACHE_POSITIONS + 1).astype(jnp.int32)
    longest = longest_request(key)
    return jnp.where(jnp.arange(INSERTED_SLOTS, dtype=jnp.int32) == longest, CACHE_POSITIONS, drawn).astype(jnp.int32)


def draw_cache_len(key, part):
    return cache_lengths(key)


def draw_inserted_key_value(key, part):
    return inserted_rows(key).astype(jnp.bfloat16)


def draw_cache_kv(key, part):
    every_entry = jax.vmap(lambda slot_entry: rows_per_slot(key, slot_entry))(jnp.arange(SLOTS, dtype=jnp.int32))
    return jnp.transpose(every_entry, (1, 0, 2, 3)).astype(jnp.bfloat16)


def draw_queries(key, part):
    base = jnp.clip(1.5 * jax.random.normal(jax.random.fold_in(key, 21), (SLOTS, QUERY_HEADS * HEAD_SIZE), jnp.float32), -9.0, 9.0)
    longest = longest_request(key)
    target_slot = slot_order(key)[longest]
    final_keys = inserted_rows(key)[0, longest, CACHE_POSITIONS // 2 - 1].astype(jnp.bfloat16).astype(jnp.float32).reshape(KEY_VALUE_HEADS, 1, HEAD_SIZE)
    final_query = jnp.broadcast_to(4.0 * final_keys, (KEY_VALUE_HEADS, QUERY_HEADS // KEY_VALUE_HEADS, HEAD_SIZE)).reshape(QUERY_HEADS * HEAD_SIZE)
    base = base.at[target_slot].set(final_query)
    return base.astype(jnp.bfloat16)


def levels(stream_key, extent, cuts, low, largest):
    def one(axis_at, shards_of):
        draws = jax.random.uniform(jax.random.fold_in(jax.random.fold_in(stream_key, 6), axis_at), (shards_of,), jnp.float32, low / len(cuts), largest / len(cuts))
        return jnp.repeat(jnp.exp(draws), extent[axis_at] // shards_of).reshape((-1,) + (1,) * (len(extent) - axis_at - 1))

    level = one(*cuts[0])
    for cut in cuts[1:]:
        level = level * one(*cut)
    return level


def choose_distinct(stream_key, rows, count, top, lift):
    sequence = jax.random.permutation(jax.random.fold_in(stream_key, 1), count)
    boost = sequence
    for power in range(3):
        boost = boost * boost // count
    boost = boost * lift // count
    tickets = jax.random.randint(jax.random.fold_in(stream_key, 2), (rows, count), 0, 4096) + boost
    sure = jax.random.permutation(jax.random.fold_in(stream_key, 3), rows)[jnp.arange(count) % rows]
    tickets = jnp.where(jnp.arange(rows)[:, None] == sure[None, :], 1 << 14, tickets)
    priority = tickets * count + jnp.arange(count)
    return lax.top_k(priority.astype(jnp.int32), top)[1].astype(jnp.int32)


def bell_draw(stream_key, shape, deviation, reach, split=(), held_as=jnp.bfloat16):
    factor_of = levels(stream_key, shape, split, -0.22, 0.18) if split else 1.0
    result = jax.random.normal(stream_key, shape, jnp.float32) * deviation * factor_of
    return jnp.minimum(jnp.maximum(result, -reach), reach).astype(held_as)


def setup_inputs(seed: int = 0, part: int = 0) -> dict:
    splits = jax.random.split(jax.random.key(seed), 14)
    part_splits = jax.random.split(jax.random.fold_in(splits[13], part), 14)
    return {
        "hidden": bell_draw(part_splits[0], (SLOTS, D), 0.3, 4.0, ((1, 16),)),
        "queries": draw_queries(jax.random.fold_in(jax.random.fold_in(splits[13], part), 71), part),
        "cache_kv": draw_cache_kv(jax.random.fold_in(jax.random.fold_in(splits[13], part), 71), part),
        "cache_len": draw_cache_len(jax.random.fold_in(jax.random.fold_in(splits[13], part), 71), part),
        "inserted_key_value": draw_inserted_key_value(jax.random.fold_in(jax.random.fold_in(splits[13], part), 71), part),
        "insert_slot": draw_insert_slot(jax.random.fold_in(jax.random.fold_in(splits[13], part), 71), part),
        "prefix_len": draw_prefix_len(jax.random.fold_in(jax.random.fold_in(splits[13], part), 71), part),
        "out_weight": bell_draw(splits[7], (QUERY_HEADS * HEAD_SIZE, D), (QUERY_HEADS * HEAD_SIZE) ** -0.5, 0.09375, ((1, 16),)),
        "norm_gain": jnp.clip(1.0 + 0.15 * jax.random.normal(splits[8], (D,), jnp.float32), 0.25, 1.75).astype(jnp.bfloat16),
        "router_weight": bell_draw(splits[9], (D, EXPERTS), D ** -0.5, 0.09375),
        "expert_ids": choose_distinct(part_splits[10], SLOTS, EXPERTS, 2, 8192),
        "gate_up": bell_draw(splits[11], (2, D, EXPERTS * FF), D ** -0.5, 0.09375, ((2, 16),)),
        "down_proj": bell_draw(splits[12], (EXPERTS * FF, D), FF ** -0.5, 0.0625, ((0, 16),)),
    }


def attend(queries, key_rows, value_rows, slot_lengths):
    slot_list = queries.shape[0]
    query_groups = QUERY_HEADS // KEY_VALUE_HEADS
    heads_of_queries = queries.astype(jnp.float32).reshape(slot_list, KEY_VALUE_HEADS, query_groups, HEAD_SIZE)
    heads_of_keys = key_rows.astype(jnp.float32).reshape(slot_list, -1, KEY_VALUE_HEADS, HEAD_SIZE)
    heads_of_values = value_rows.astype(jnp.float32).reshape(slot_list, -1, KEY_VALUE_HEADS, HEAD_SIZE)
    scores = jnp.einsum('skgd,sckd->skgc', heads_of_queries, heads_of_keys) / math.sqrt(HEAD_SIZE)
    positions = jnp.arange(heads_of_keys.shape[1], dtype=jnp.int32)
    masked = (positions[None, :] < slot_lengths[:, None])[:, None, None, :]
    scores = jnp.where(masked, scores, -1e+30)
    peak = lax.optimization_barrier(jnp.max(scores, axis=-1, keepdims=True))
    weights = jnp.where(masked, jnp.exp(scores - peak), 0.0)
    totals = lax.optimization_barrier(jnp.sum(weights, axis=-1))
    mixed_values = jnp.einsum('skgc,sckd->skgd', weights, heads_of_values)
    return (mixed_values / totals[..., None]).reshape(slot_list, QUERY_HEADS * HEAD_SIZE)

def route_shares(normed, router_weight, expert_ids):
    logits = jnp.dot(normed, router_weight, preferred_element_type=jnp.float32)
    chosen = (expert_ids[:, :, None] == jnp.arange(EXPERTS, dtype=jnp.int32)[None, None, :]).astype(jnp.float32)
    picked = lax.optimization_barrier(jnp.sum(chosen * logits[:, None, :], axis=-1))
    gates = jax.nn.sigmoid(picked - picked[:, ::-1])
    return lax.optimization_barrier(jnp.sum(gates[:, :, None] * chosen, axis=1))

def reference(hidden, queries, cache_kv, cache_len, inserted_key_value, insert_slot, prefix_len, out_weight, norm_gain, router_weight, expert_ids, gate_up, down_proj):
    placed = jnp.roll(inserted_key_value, CACHE_POSITIONS // 2, axis=2)
    cache = cache_kv.at[:, insert_slot].set(placed)
    slot_lengths = cache_len.at[insert_slot].set(prefix_len)
    attn = attend(queries, cache[0], cache[1], slot_lengths).astype(jnp.bfloat16)
    mixed = (hidden.astype(jnp.float32) + jnp.dot(attn, out_weight, preferred_element_type=jnp.float32)).astype(jnp.bfloat16)
    mixed_f = mixed.astype(jnp.float32)
    scale = jax.lax.rsqrt(lax.optimization_barrier(jnp.mean(mixed_f * mixed_f, axis=-1, keepdims=True)) + 1e-05)
    normed = (mixed_f * scale * norm_gain.astype(jnp.float32)).astype(jnp.bfloat16)
    shares = route_shares(normed, router_weight, expert_ids)
    moe = jnp.zeros(mixed_f.shape, jnp.float32)
    for expert in range(EXPERTS):
        gate_part = gate_up[0][:, expert * FF:(expert + 1) * FF]
        up_part = gate_up[1][:, expert * FF:(expert + 1) * FF]
        act = (jax.nn.silu(jnp.dot(normed, gate_part, preferred_element_type=jnp.float32)) * jnp.dot(normed, up_part, preferred_element_type=jnp.float32)).astype(jnp.bfloat16)
        moe = moe + shares[:, expert:expert + 1] * jnp.dot(act, down_proj[expert * FF:(expert + 1) * FF], preferred_element_type=jnp.float32)
    return (mixed_f + moe).astype(jnp.bfloat16)
```

```python
import functools
import math

import jax
import jax.numpy as jnp
from jax import lax
from jax.experimental import pallas as pl
from jax.experimental.pallas import tpu as pltpu
from jax.sharding import PartitionSpec as P

QUERY_HEADS = 32
KEY_VALUE_HEADS = 8
HEAD_SIZE = 128
EXPERTS = 4
FF = 7168


def merged(value, axis, join):
    pieces = jax.tree.map(lambda part: lax.all_gather(part, axis), value)
    head = jax.tree.map(lambda part: part[0], pieces)
    tail = jax.tree.map(lambda part: part[1:], pieces)
    total, _ = lax.scan(lambda total, piece: (join(total, piece), None), head, tail)
    return total


def block_attention(queries, key_rows, value_rows, valid):
    slot_list = queries.shape[0]
    query_groups = QUERY_HEADS // KEY_VALUE_HEADS
    heads_of_queries = queries.astype(jnp.float32).reshape(
        slot_list, KEY_VALUE_HEADS, query_groups, HEAD_SIZE
    )
    heads_of_keys = key_rows.astype(jnp.float32).reshape(slot_list, -1, KEY_VALUE_HEADS, HEAD_SIZE)
    heads_of_values = value_rows.astype(jnp.float32).reshape(
        slot_list, -1, KEY_VALUE_HEADS, HEAD_SIZE
    )
    scores = jnp.einsum("skgd,sckd->skgc", heads_of_queries, heads_of_keys) / math.sqrt(HEAD_SIZE)
    masked = valid[:, None, None, :]
    peak = jnp.max(jnp.where(masked, scores, -1e30), axis=-1)
    weights = jnp.where(masked, jnp.exp(scores - peak[..., None]), 0.0)
    totals = jnp.sum(weights, axis=-1)
    partial_value = jnp.einsum("skgc,sckd->skgd", weights, heads_of_values)
    return (
        partial_value.reshape(slot_list, QUERY_HEADS, HEAD_SIZE),
        peak.reshape(slot_list, QUERY_HEADS),
        totals.reshape(slot_list, QUERY_HEADS),
    )


def merge_pair(earlier, later):
    early_out, early_peak, early_total = earlier
    late_out, late_peak, late_total = later
    highest = jnp.maximum(early_peak, late_peak)
    early_scale = jnp.exp(early_peak - highest)
    late_scale = jnp.exp(late_peak - highest)
    merged_out = early_out * early_scale[..., None] + late_out * late_scale[..., None]
    return (merged_out, highest, early_total * early_scale + late_total * late_scale)


def route_shares(normed, router_weight, expert_ids):
    logits = jnp.dot(normed, router_weight, preferred_element_type=jnp.float32)
    chosen = (expert_ids[:, :, None] == jnp.arange(EXPERTS, dtype=jnp.int32)[None, None, :]).astype(
        jnp.float32
    )
    picked = jnp.sum(chosen * logits[:, None, :], axis=-1)
    gates = jax.nn.sigmoid(picked - picked[:, ::-1])
    return jnp.sum(gates[:, :, None] * chosen, axis=1)


def plain_layer(
    hidden,
    queries,
    cache_kv,
    cache_len,
    inserted_key_value,
    insert_slot,
    prefix_len,
    out_weight,
    norm_gain,
    router_weight,
    expert_ids,
    gate_up,
    down_proj,
):
    cycle_size = lax.axis_size("blk")
    dev_index = lax.axis_index("blk")
    ctx_rows = cache_kv.shape[2]
    half = cycle_size * ctx_rows // 2
    cache = cache_kv.at[:, insert_slot].set(inserted_key_value)
    slot_lengths = cache_len.at[insert_slot].set(prefix_len)
    positions = dev_index * ctx_rows + jnp.arange(ctx_rows, dtype=jnp.int32)
    rolled = jnp.where(positions < half, positions + half, positions - half)
    inserted = jnp.zeros(cache_len.shape, jnp.bool_).at[insert_slot].set(True)
    held = jnp.where(inserted[:, None], rolled[None, :], positions[None, :])
    valid = held < slot_lengths[:, None]
    partial_value, peak, totals = block_attention(queries, cache[0], cache[1], valid)
    slot_list = queries.shape[0]
    summed, highest, all_totals = merged((partial_value, peak, totals), "blk", merge_pair)
    attn = (
        (summed / all_totals[..., None])
        .reshape(slot_list, QUERY_HEADS * HEAD_SIZE)
        .astype(jnp.bfloat16)
    )
    local_mixed = (
        hidden.astype(jnp.float32) + jnp.dot(attn, out_weight, preferred_element_type=jnp.float32)
    ).astype(jnp.bfloat16)
    mixed = lax.all_gather(local_mixed, "blk", axis=1, tiled=True)
    mixed_f = mixed.astype(jnp.float32)
    scale = lax.rsqrt(jnp.mean(mixed_f * mixed_f, axis=-1, keepdims=True) + 1e-05)
    normed = (mixed_f * scale * norm_gain.astype(jnp.float32)).astype(jnp.bfloat16)
    shares = route_shares(normed, router_weight, expert_ids)
    unit_count = gate_up.shape[2]
    expert_now = dev_index * unit_count // FF
    picker = (jnp.arange(EXPERTS, dtype=jnp.int32) == expert_now).astype(jnp.float32)
    expert_share = jnp.sum(shares * picker[None, :], axis=1)
    act = (
        jax.nn.silu(jnp.dot(normed, gate_up[0], preferred_element_type=jnp.float32))
        * jnp.dot(normed, gate_up[1], preferred_element_type=jnp.float32)
    ).astype(jnp.bfloat16)
    term = expert_share[:, None] * jnp.dot(act, down_proj, preferred_element_type=jnp.float32)
    moe = lax.psum_scatter(term, "blk", scatter_dimension=1, tiled=True)
    return (local_mixed.astype(jnp.float32) + moe).astype(jnp.bfloat16)


NEG = -1e30
GU_CHUNKS = 8
MESH = pl.DeviceIdType.MESH


def fused_kernel(
    n,
    cache_len,
    insert_slot,
    prefix_len,
    expert_ids,
    hidden_h,
    queries_h,
    cache_h,
    inserted_h,
    out_w_h,
    gain_h,
    router_h,
    gate_up_h,
    down_h,
    out_ref,
    hidden,
    queries,
    kv,
    out_w,
    gain,
    router,
    gate_up,
    down,
    part_send,
    part_recv,
    attn_all,
    mixed_all,
    normed_ref,
    gate_acc,
    up_acc,
    term_send,
    term_recv,
    in_sem,
    gu_sem,
    down_sem,
    send_sem,
    recv_sem,
):
    me = lax.axis_index("blk")
    slots = queries.shape[0]
    group = QUERY_HEADS // KEY_VALUE_HEADS
    inserts = insert_slot.shape[0]
    ctx = kv.shape[2]
    width = out_w.shape[1]
    depth = gate_up.shape[1] // GU_CHUNKS
    units = gate_up.shape[2]

    copies = [
        pltpu.make_async_copy(s, d, in_sem.at[i])
        for i, (s, d) in enumerate(
            [
                (queries_h, queries),
                (cache_h, kv.at[:, pl.ds(0, slots)]),
                (inserted_h, kv.at[:, pl.ds(slots, inserts)]),
                (hidden_h, hidden),
                (gain_h, gain),
                (router_h, router),
                (out_w_h, out_w),
            ]
        )
    ]
    for copy in copies:
        copy.start()

    def gu_copy(k):
        rows = pl.ds(pl.multiple_of(k * depth, depth), depth)
        return pltpu.make_async_copy(gate_up_h.at[:, rows], gate_up.at[:, rows], gu_sem.at[k])

    def columns(c):
        return pl.ds(pl.multiple_of(c * width, width), width)

    def down_copy(c):
        return pltpu.make_async_copy(
            down_h.at[:, columns(c)], down.at[:, columns(c)], down_sem.at[c]
        )

    def each(count, step):
        lax.fori_loop(0, count, lambda i, carry: (step(i), carry)[1], 0)

    def peer_of(i):
        return lax.rem(me + 1 + i, n)

    barrier = pltpu.get_barrier_semaphore()
    each(
        n - 1,
        lambda i: pl.semaphore_signal(
            barrier, inc=1, device_id={"blk": peer_of(i)}, device_id_type=MESH
        ),
    )
    each(GU_CHUNKS, lambda k: gu_copy(k).start())
    each(n, lambda i: down_copy(peer_of(i)).start())

    entries = slots + inserts
    cols = entries * ctx
    col = lax.broadcasted_iota(jnp.int32, (1, cols), 1)
    shift = ctx.bit_length() - 1
    entry = lax.shift_right_logical(col, jnp.full_like(col, shift))
    row_at = me * ctx + (col & (ctx - 1))
    half = n * ctx // 2
    rolled = jnp.where(row_at < half, row_at + half, row_at - half)
    position = jnp.where(entry < slots, row_at, rolled)
    slot_of = entry
    length = jnp.zeros_like(col)
    for s in range(slots):
        length = jnp.where(entry == s, cache_len[s], length)
    for j in range(inserts):
        slot_of = jnp.where(entry == insert_slot[j], -1, slot_of)
    for j in range(inserts):
        slot_of = jnp.where(entry == slots + j, insert_slot[j], slot_of)
        length = jnp.where(entry == slots + j, prefix_len[j], length)
    slot_of = jnp.where(position < length, slot_of, -1)
    rows = group * slots
    row_slot = lax.broadcasted_iota(jnp.int32, (rows, 1), 0) & (slots - 1)
    mask = row_slot == slot_of
    lane = lax.broadcasted_iota(jnp.int32, (rows, HEAD_SIZE), 1)
    place = lane & (HEAD_SIZE // 2 - 1)
    low_lane = lane[:slots] < HEAD_SIZE // 2

    for copy in copies[:3]:
        copy.wait()
    per_group = group // 2
    for g in range(KEY_VALUE_HEADS):
        q = jnp.concatenate(
            [
                queries[:, (g * group + r) * HEAD_SIZE : (g * group + r + 1) * HEAD_SIZE]
                for r in range(group)
            ],
            axis=0,
        )
        span = slice(g * HEAD_SIZE, (g + 1) * HEAD_SIZE)
        keys = kv[0, :, :, span].reshape(cols, HEAD_SIZE)
        values = kv[1, :, :, span].reshape(cols, HEAD_SIZE)
        scores = lax.dot_general(
            q, keys, (((1,), (1,)), ((), ())), preferred_element_type=jnp.float32
        ) * (1.0 / math.sqrt(HEAD_SIZE))
        peak = jnp.max(jnp.where(mask, scores, NEG), axis=-1, keepdims=True)
        peak = peak.astype(jnp.bfloat16).astype(jnp.float32)
        weights = jnp.where(mask, jnp.exp(scores - peak), 0.0).astype(jnp.bfloat16)
        total = jnp.sum(weights.astype(jnp.float32), axis=-1, keepdims=True)
        summed = jnp.dot(weights, values, preferred_element_type=jnp.float32)
        total_high = total.astype(jnp.bfloat16).astype(jnp.float32)
        stats = jnp.where(
            place == 0, peak, jnp.where(place == 1, total_high, total - total_high)
        )
        for h in range(per_group):
            at = 2 * h * slots
            c = g * per_group + h
            part_send[c, 0 : 2 * slots, :] = summed[at : at + 2 * slots].astype(jnp.bfloat16)
            part_send[c, 2 * slots : 3 * slots, :] = jnp.where(
                low_lane, stats[at : at + slots], stats[at + slots : at + 2 * slots]
            ).astype(jnp.bfloat16)
    part_recv[me] = part_send[me]

    pl.semaphore_wait(barrier, n - 1)

    def part_copy(to, slot):
        return pltpu.make_async_remote_copy(
            src_ref=part_send.at[to],
            dst_ref=part_recv.at[slot],
            send_sem=send_sem.at[0, to],
            recv_sem=recv_sem.at[0, slot],
            device_id={"blk": to},
            device_id_type=MESH,
        )

    def share_copy(ref, phase, to, slot):
        return pltpu.make_async_remote_copy(
            src_ref=ref.at[:, columns(slot)],
            dst_ref=ref.at[:, columns(slot)],
            send_sem=send_sem.at[phase, to],
            recv_sem=recv_sem.at[phase, slot],
            device_id={"blk": to},
            device_id_type=MESH,
        )

    def term_copy(to, slot):
        return pltpu.make_async_remote_copy(
            src_ref=term_send.at[to],
            dst_ref=term_recv.at[slot],
            send_sem=send_sem.at[3, to],
            recv_sem=recv_sem.at[3, slot],
            device_id={"blk": to},
            device_id_type=MESH,
        )

    each(n - 1, lambda i: part_copy(peer_of(i), me).start())
    each(n - 1, lambda i: part_copy(peer_of(i), peer_of(i)).wait_recv())

    stat_parts = [part_recv[i, 2 * slots : 3 * slots, :].astype(jnp.float32) for i in range(n)]
    highest = functools.reduce(jnp.maximum, stat_parts)
    sums = [jnp.zeros((slots, HEAD_SIZE), jnp.float32) for _ in range(2)]
    totals = [jnp.zeros((slots, 1), jnp.float32) for _ in range(2)]
    for i in range(n):
        scale = jnp.exp(stat_parts[i] - highest)
        for h in range(2):
            at = h * (HEAD_SIZE // 2)
            weight = scale[:, at : at + 1]
            totals[h] += weight * (
                stat_parts[i][:, at + 1 : at + 2] + stat_parts[i][:, at + 2 : at + 3]
            )
            sums[h] += weight * part_recv[i, h * slots : (h + 1) * slots, :].astype(jnp.float32)
    attn = jnp.concatenate([sums[h] / totals[h] for h in range(2)], axis=1)
    attn_all[:, columns(me)] = attn.astype(jnp.bfloat16)
    each(n - 1, lambda i: share_copy(attn_all, 1, peer_of(i), me).start())
    for copy in copies[3:]:
        copy.wait()
    each(n - 1, lambda i: share_copy(attn_all, 1, peer_of(i), peer_of(i)).wait_recv())

    local_mixed = (
        hidden[...].astype(jnp.float32)
        + jnp.dot(attn_all[...], out_w[...], preferred_element_type=jnp.float32)
    ).astype(jnp.bfloat16)
    mixed_all[:, columns(me)] = local_mixed
    each(n - 1, lambda i: share_copy(mixed_all, 2, peer_of(i), me).start())
    each(n - 1, lambda i: share_copy(mixed_all, 2, peer_of(i), peer_of(i)).wait_recv())

    mixed = mixed_all[...].astype(jnp.float32)
    scale = lax.rsqrt(jnp.mean(mixed * mixed, axis=-1, keepdims=True) + 1e-05)
    normed = (mixed * scale * gain[...].astype(jnp.float32)).astype(jnp.bfloat16)
    normed_ref[...] = normed
    normed = normed.astype(jnp.float32)
    router_rows = router[...].astype(jnp.float32)
    logits = [
        jnp.sum(normed * router_rows[e : e + 1], axis=-1, keepdims=True) for e in range(EXPERTS)
    ]
    row = lax.broadcasted_iota(jnp.int32, (slots, 1), 0)
    chosen = []
    for k in range(2):
        ids = jnp.zeros_like(row)
        for s in range(slots):
            ids = jnp.where(row == s, expert_ids[2 * s + k], ids)
        chosen.append(ids)
    picked = [
        sum(jnp.where(chosen[k] == e, logits[e], 0.0) for e in range(EXPERTS)) for k in range(2)
    ]
    expert_now = (me * units) // FF
    share = jnp.where(chosen[0] == expert_now, jax.nn.sigmoid(picked[0] - picked[1]), 0.0)
    share += jnp.where(chosen[1] == expert_now, jax.nn.sigmoid(picked[1] - picked[0]), 0.0)

    gate_acc[...] = jnp.zeros_like(gate_acc)
    up_acc[...] = jnp.zeros_like(up_acc)

    def gu_step(k):
        gu_copy(k).wait()
        rows = pl.ds(pl.multiple_of(k * depth, depth), depth)
        piece = normed_ref[:, rows]
        gate_acc[...] += jnp.dot(piece, gate_up[0, rows, :], preferred_element_type=jnp.float32)
        up_acc[...] += jnp.dot(piece, gate_up[1, rows, :], preferred_element_type=jnp.float32)

    each(GU_CHUNKS, gu_step)
    gate = gate_acc[...]
    act = (gate * jax.nn.sigmoid(gate) * up_acc[...]).astype(jnp.bfloat16)

    def term_of(c):
        down_copy(c).wait()
        return share * jnp.dot(act, down[:, columns(c)], preferred_element_type=jnp.float32)

    def term_step(i):
        c = peer_of(i)
        term_send[c] = term_of(c).astype(jnp.bfloat16)
        term_copy(c, me).start()

    each(n - 1, term_step)
    total = local_mixed.astype(jnp.float32) + term_of(me)
    term_recv[me] = jnp.zeros((slots, width), jnp.bfloat16)
    each(n - 1, lambda i: term_copy(peer_of(i), peer_of(i)).wait_recv())
    for i in range(n):
        total += term_recv[i].astype(jnp.float32)
    out_ref[...] = total.astype(jnp.bfloat16)

    def drain(i):
        c = peer_of(i)
        part_copy(c, me).wait_send()
        share_copy(attn_all, 1, c, me).wait_send()
        share_copy(mixed_all, 2, c, me).wait_send()
        term_copy(c, me).wait_send()

    each(n - 1, drain)


def fused_layer(
    n,
    hidden,
    queries,
    cache_kv,
    cache_len,
    inserted_key_value,
    insert_slot,
    prefix_len,
    out_weight,
    norm_gain,
    router_weight,
    expert_ids,
    gate_up,
    down_proj,
):
    slots, features = queries.shape
    entries = slots + insert_slot.shape[0]
    width = out_weight.shape[1]
    units = gate_up.shape[2]
    any_space = pl.BlockSpec(memory_space=pl.ANY)
    smem = pl.BlockSpec(memory_space=pltpu.SMEM)
    bf16, f32 = jnp.bfloat16, jnp.float32
    return pl.pallas_call(
        functools.partial(fused_kernel, n),
        out_shape=jax.ShapeDtypeStruct((slots, width), bf16),
        in_specs=[smem] * 4 + [any_space] * 9,
        out_specs=pl.BlockSpec(memory_space=pltpu.VMEM),
        scratch_shapes=[
            pltpu.VMEM((slots, width), bf16),
            pltpu.VMEM((slots, features), bf16),
            pltpu.VMEM((2, entries) + cache_kv.shape[2:], bf16),
            pltpu.VMEM(out_weight.shape, bf16),
            pltpu.VMEM((1, features), bf16),
            pltpu.VMEM((EXPERTS, features), bf16),
            pltpu.VMEM(gate_up.shape, bf16),
            pltpu.VMEM(down_proj.shape, bf16),
            pltpu.VMEM((n, 3 * slots, HEAD_SIZE), bf16),
            pltpu.VMEM((n, 3 * slots, HEAD_SIZE), bf16),
            pltpu.VMEM((slots, features), bf16),
            pltpu.VMEM((slots, features), bf16),
            pltpu.VMEM((slots, features), bf16),
            pltpu.VMEM((slots, units), f32),
            pltpu.VMEM((slots, units), f32),
            pltpu.VMEM((n, slots, width), bf16),
            pltpu.VMEM((n, slots, width), bf16),
            pltpu.SemaphoreType.DMA((7,)),
            pltpu.SemaphoreType.DMA((GU_CHUNKS,)),
            pltpu.SemaphoreType.DMA((n,)),
            pltpu.SemaphoreType.DMA((4, n)),
            pltpu.SemaphoreType.DMA((4, n)),
        ],
        compiler_params=pltpu.CompilerParams(
            collective_id=0, has_side_effects=True, vmem_limit_bytes=60 * 1024 * 1024
        ),
        name="layer",
    )(
        cache_len,
        insert_slot,
        prefix_len,
        expert_ids.reshape(-1),
        hidden,
        queries,
        cache_kv,
        inserted_key_value,
        out_weight,
        norm_gain.reshape(1, features),
        router_weight.T,
        gate_up,
        down_proj,
    )


def on_device(*args):
    n = lax.axis_size("blk")
    queries, cache_kv, out_weight, gate_up = args[1], args[2], args[7], args[11]
    ctx, slots = cache_kv.shape[2], queries.shape[0]
    fits = (
        QUERY_HEADS == 2 * n
        and out_weight.shape[1] == 2 * HEAD_SIZE
        and ctx % 16 == 0
        and ctx & (ctx - 1) == 0
        and slots % 16 == 0
        and slots & (slots - 1) == 0
        and gate_up.shape[1] % (128 * GU_CHUNKS) == 0
        and gate_up.shape[2] % 128 == 0
        and FF % gate_up.shape[2] == 0
    )
    return fused_layer(n, *args) if fits else plain_layer(*args)


def solution(mesh):
    in_specs = (
        P("rep", "blk"),
        P("rep", None),
        P(None, "rep", "blk", None),
        P("rep"),
        P(None, "rep", "blk", None),
        P("rep"),
        P("rep"),
        P(None, "blk"),
        P(),
        P(),
        P("rep", None),
        P(None, None, "blk"),
        P("blk", None),
    )
    out_specs = P("rep", "blk")
    return jax.shard_map(
        on_device, mesh=mesh, in_specs=in_specs, out_specs=out_specs, check_vma=False
    )
```

```python
import functools
import math

import jax
import jax.numpy as jnp
from jax import lax
from jax.experimental import pallas as pl
from jax.experimental.pallas import tpu as pltpu
from jax.sharding import PartitionSpec as P

QUERY_HEADS = 32
KEY_VALUE_HEADS = 8
HEAD_SIZE = 128
EXPERTS = 4
FF = 7168


def merged(value, axis, join):
    pieces = jax.tree.map(lambda part: lax.all_gather(part, axis), value)
    head = jax.tree.map(lambda part: part[0], pieces)
    tail = jax.tree.map(lambda part: part[1:], pieces)
    total, _ = lax.scan(lambda total, piece: (join(total, piece), None), head, tail)
    return total


def block_attention(queries, key_rows, value_rows, valid):
    slot_list = queries.shape[0]
    query_groups = QUERY_HEADS // KEY_VALUE_HEADS
    heads_of_queries = queries.astype(jnp.float32).reshape(
        slot_list, KEY_VALUE_HEADS, query_groups, HEAD_SIZE
    )
    heads_of_keys = key_rows.astype(jnp.float32).reshape(slot_list, -1, KEY_VALUE_HEADS, HEAD_SIZE)
    heads_of_values = value_rows.astype(jnp.float32).reshape(
        slot_list, -1, KEY_VALUE_HEADS, HEAD_SIZE
    )
    scores = jnp.einsum("skgd,sckd->skgc", heads_of_queries, heads_of_keys) / math.sqrt(HEAD_SIZE)
    masked = valid[:, None, None, :]
    peak = jnp.max(jnp.where(masked, scores, -1e30), axis=-1)
    weights = jnp.where(masked, jnp.exp(scores - peak[..., None]), 0.0)
    totals = jnp.sum(weights, axis=-1)
    partial_value = jnp.einsum("skgc,sckd->skgd", weights, heads_of_values)
    return (
        partial_value.reshape(slot_list, QUERY_HEADS, HEAD_SIZE),
        peak.reshape(slot_list, QUERY_HEADS),
        totals.reshape(slot_list, QUERY_HEADS),
    )


def merge_pair(earlier, later):
    early_out, early_peak, early_total = earlier
    late_out, late_peak, late_total = later
    highest = jnp.maximum(early_peak, late_peak)
    early_scale = jnp.exp(early_peak - highest)
    late_scale = jnp.exp(late_peak - highest)
    merged_out = early_out * early_scale[..., None] + late_out * late_scale[..., None]
    return (merged_out, highest, early_total * early_scale + late_total * late_scale)


def route_shares(normed, router_weight, expert_ids):
    logits = jnp.dot(normed, router_weight, preferred_element_type=jnp.float32)
    chosen = (expert_ids[:, :, None] == jnp.arange(EXPERTS, dtype=jnp.int32)[None, None, :]).astype(
        jnp.float32
    )
    picked = jnp.sum(chosen * logits[:, None, :], axis=-1)
    gates = jax.nn.sigmoid(picked - picked[:, ::-1])
    return jnp.sum(gates[:, :, None] * chosen, axis=1)


def plain_layer(
    hidden,
    queries,
    cache_kv,
    cache_len,
    inserted_key_value,
    insert_slot,
    prefix_len,
    out_weight,
    norm_gain,
    router_weight,
    expert_ids,
    gate_up,
    down_proj,
):
    cycle_size = lax.axis_size("blk")
    dev_index = lax.axis_index("blk")
    ctx_rows = cache_kv.shape[2]
    half = cycle_size * ctx_rows // 2
    cache = cache_kv.at[:, insert_slot].set(inserted_key_value)
    slot_lengths = cache_len.at[insert_slot].set(prefix_len)
    positions = dev_index * ctx_rows + jnp.arange(ctx_rows, dtype=jnp.int32)
    rolled = jnp.where(positions < half, positions + half, positions - half)
    inserted = jnp.zeros(cache_len.shape, jnp.bool_).at[insert_slot].set(True)
    held = jnp.where(inserted[:, None], rolled[None, :], positions[None, :])
    valid = held < slot_lengths[:, None]
    partial_value, peak, totals = block_attention(queries, cache[0], cache[1], valid)
    slot_list = queries.shape[0]
    summed, highest, all_totals = merged((partial_value, peak, totals), "blk", merge_pair)
    attn = (
        (summed / all_totals[..., None])
        .reshape(slot_list, QUERY_HEADS * HEAD_SIZE)
        .astype(jnp.bfloat16)
    )
    local_mixed = (
        hidden.astype(jnp.float32) + jnp.dot(attn, out_weight, preferred_element_type=jnp.float32)
    ).astype(jnp.bfloat16)
    mixed = lax.all_gather(local_mixed, "blk", axis=1, tiled=True)
    mixed_f = mixed.astype(jnp.float32)
    scale = lax.rsqrt(jnp.mean(mixed_f * mixed_f, axis=-1, keepdims=True) + 1e-05)
    normed = (mixed_f * scale * norm_gain.astype(jnp.float32)).astype(jnp.bfloat16)
    shares = route_shares(normed, router_weight, expert_ids)
    unit_count = gate_up.shape[2]
    expert_now = dev_index * unit_count // FF
    picker = (jnp.arange(EXPERTS, dtype=jnp.int32) == expert_now).astype(jnp.float32)
    expert_share = jnp.sum(shares * picker[None, :], axis=1)
    act = (
        jax.nn.silu(jnp.dot(normed, gate_up[0], preferred_element_type=jnp.float32))
        * jnp.dot(normed, gate_up[1], preferred_element_type=jnp.float32)
    ).astype(jnp.bfloat16)
    term = expert_share[:, None] * jnp.dot(act, down_proj, preferred_element_type=jnp.float32)
    moe = lax.psum_scatter(term, "blk", scatter_dimension=1, tiled=True)
    return (local_mixed.astype(jnp.float32) + moe).astype(jnp.bfloat16)


NEG = -1e30
GU_CHUNKS = 8
MESH = pl.DeviceIdType.MESH


def fused_kernel(
    n,
    cache_len,
    insert_slot,
    prefix_len,
    expert_ids,
    hidden_h,
    queries_h,
    cache_h,
    inserted_h,
    out_w_h,
    gain_h,
    router_h,
    gate_up_h,
    down_h,
    out_ref,
    hidden,
    queries,
    kv,
    out_w,
    gain,
    router,
    gate_up,
    down,
    part_send,
    part_recv,
    attn_all,
    mixed_all,
    normed_ref,
    gate_acc,
    up_acc,
    term_send,
    term_recv,
    in_sem,
    gu_sem,
    down_sem,
    send_sem,
    recv_sem,
):
    me = lax.axis_index("blk")
    slots = queries.shape[0]
    group = QUERY_HEADS // KEY_VALUE_HEADS
    inserts = insert_slot.shape[0]
    ctx = kv.shape[2]
    width = out_w.shape[1]
    depth = gate_up.shape[1] // GU_CHUNKS
    units = gate_up.shape[2]

    copies = [
        pltpu.make_async_copy(s, d, in_sem.at[i])
        for i, (s, d) in enumerate(
            [
                (queries_h, queries),
                (cache_h, kv.at[:, pl.ds(0, slots)]),
                (inserted_h, kv.at[:, pl.ds(slots, inserts)]),
                (hidden_h, hidden),
                (gain_h, gain),
                (router_h, router),
                (out_w_h, out_w),
            ]
        )
    ]
    for copy in copies:
        copy.start()

    def gu_copy(k):
        rows = pl.ds(pl.multiple_of(k * depth, depth), depth)
        return pltpu.make_async_copy(gate_up_h.at[:, rows], gate_up.at[:, rows], gu_sem.at[k])

    def columns(c):
        return pl.ds(pl.multiple_of(c * width, width), width)

    def down_copy(c):
        return pltpu.make_async_copy(
            down_h.at[:, columns(c)], down.at[:, columns(c)], down_sem.at[c]
        )

    def every(count, step):
        for i in range(count):
            step(i)

    def each(count, step):
        lax.fori_loop(0, count, lambda i, carry: (step(i), carry)[1], 0)

    def peer_of(i):
        later = me + 1 + i
        return jnp.where(later >= n, later - n, later)

    barrier = pltpu.get_barrier_semaphore()
    every(
        n - 1,
        lambda i: pl.semaphore_signal(
            barrier, inc=1, device_id={"blk": peer_of(i)}, device_id_type=MESH
        ),
    )
    each(GU_CHUNKS, lambda k: gu_copy(k).start())
    each(n, lambda i: down_copy(peer_of(i)).start())

    entries = slots + inserts
    cols = entries * ctx
    col = lax.broadcasted_iota(jnp.int32, (1, cols), 1)
    shift = ctx.bit_length() - 1
    entry = lax.shift_right_logical(col, jnp.full_like(col, shift))
    row_at = me * ctx + (col & (ctx - 1))
    half = n * ctx // 2
    rolled = jnp.where(row_at < half, row_at + half, row_at - half)
    position = jnp.where(entry < slots, row_at, rolled)
    slot_of = entry
    length = jnp.zeros_like(col)
    for s in range(slots):
        length = jnp.where(entry == s, cache_len[s], length)
    for j in range(inserts):
        slot_of = jnp.where(entry == insert_slot[j], -1, slot_of)
    for j in range(inserts):
        slot_of = jnp.where(entry == slots + j, insert_slot[j], slot_of)
        length = jnp.where(entry == slots + j, prefix_len[j], length)
    slot_of = jnp.where(position < length, slot_of, -1)
    rows = group * slots
    row_slot = lax.broadcasted_iota(jnp.int32, (rows, 1), 0) & (slots - 1)
    mask = row_slot == slot_of
    lane = lax.broadcasted_iota(jnp.int32, (rows, HEAD_SIZE), 1)
    place = lane & (HEAD_SIZE // 2 - 1)
    low_lane = lane[:slots] < HEAD_SIZE // 2

    for copy in copies[:3]:
        copy.wait()
    per_group = group // 2
    for g in range(KEY_VALUE_HEADS):
        q = jnp.concatenate(
            [
                queries[:, (g * group + r) * HEAD_SIZE : (g * group + r + 1) * HEAD_SIZE]
                for r in range(group)
            ],
            axis=0,
        )
        span = slice(g * HEAD_SIZE, (g + 1) * HEAD_SIZE)
        keys = kv[0, :, :, span].reshape(cols, HEAD_SIZE)
        values = kv[1, :, :, span].reshape(cols, HEAD_SIZE)
        scores = lax.dot_general(
            q, keys, (((1,), (1,)), ((), ())), preferred_element_type=jnp.float32
        ) * (1.0 / math.sqrt(HEAD_SIZE))
        peak = jnp.max(jnp.where(mask, scores, NEG), axis=-1, keepdims=True)
        peak = peak.astype(jnp.bfloat16).astype(jnp.float32)
        weights = jnp.where(mask, jnp.exp(scores - peak), 0.0).astype(jnp.bfloat16)
        total = jnp.sum(weights.astype(jnp.float32), axis=-1, keepdims=True)
        summed = jnp.dot(weights, values, preferred_element_type=jnp.float32)
        total_high = total.astype(jnp.bfloat16).astype(jnp.float32)
        stats = jnp.where(
            place == 0, peak, jnp.where(place == 1, total_high, total - total_high)
        )
        for h in range(per_group):
            at = 2 * h * slots
            c = g * per_group + h
            part_send[c, 0 : 2 * slots, :] = summed[at : at + 2 * slots].astype(jnp.bfloat16)
            part_send[c, 2 * slots : 3 * slots, :] = jnp.where(
                low_lane, stats[at : at + slots], stats[at + slots : at + 2 * slots]
            ).astype(jnp.bfloat16)
    part_recv[me] = part_send[me]

    pl.semaphore_wait(barrier, n - 1)

    def part_copy(to, slot):
        return pltpu.make_async_remote_copy(
            src_ref=part_send.at[to],
            dst_ref=part_recv.at[slot],
            send_sem=send_sem.at[0, to],
            recv_sem=recv_sem.at[0, slot],
            device_id={"blk": to},
            device_id_type=MESH,
        )

    def share_copy(ref, phase, to, slot):
        return pltpu.make_async_remote_copy(
            src_ref=ref.at[:, columns(slot)],
            dst_ref=ref.at[:, columns(slot)],
            send_sem=send_sem.at[phase, to],
            recv_sem=recv_sem.at[phase, slot],
            device_id={"blk": to},
            device_id_type=MESH,
        )

    def term_copy(to, slot):
        return pltpu.make_async_remote_copy(
            src_ref=term_send.at[to],
            dst_ref=term_recv.at[slot],
            send_sem=send_sem.at[3, to],
            recv_sem=recv_sem.at[3, slot],
            device_id={"blk": to},
            device_id_type=MESH,
        )

    every(n - 1, lambda i: part_copy(peer_of(i), me).start())
    every(n - 1, lambda i: part_copy(peer_of(i), peer_of(i)).wait_recv())

    stat_parts = [part_recv[i, 2 * slots : 3 * slots, :].astype(jnp.float32) for i in range(n)]
    highest = functools.reduce(jnp.maximum, stat_parts)
    sums = [jnp.zeros((slots, HEAD_SIZE), jnp.float32) for _ in range(2)]
    totals = [jnp.zeros((slots, 1), jnp.float32) for _ in range(2)]
    for i in range(n):
        scale = jnp.exp(stat_parts[i] - highest)
        for h in range(2):
            at = h * (HEAD_SIZE // 2)
            weight = scale[:, at : at + 1]
            totals[h] += weight * (
                stat_parts[i][:, at + 1 : at + 2] + stat_parts[i][:, at + 2 : at + 3]
            )
            sums[h] += weight * part_recv[i, h * slots : (h + 1) * slots, :].astype(jnp.float32)
    attn = jnp.concatenate([sums[h] / totals[h] for h in range(2)], axis=1)
    attn_all[:, columns(me)] = attn.astype(jnp.bfloat16)
    every(n - 1, lambda i: share_copy(attn_all, 1, peer_of(i), me).start())
    for copy in copies[3:]:
        copy.wait()
    every(n - 1, lambda i: share_copy(attn_all, 1, peer_of(i), peer_of(i)).wait_recv())

    local_mixed = (
        hidden[...].astype(jnp.float32)
        + jnp.dot(attn_all[...], out_w[...], preferred_element_type=jnp.float32)
    ).astype(jnp.bfloat16)
    mixed_all[:, columns(me)] = local_mixed
    every(n - 1, lambda i: share_copy(mixed_all, 2, peer_of(i), me).start())
    every(n - 1, lambda i: share_copy(mixed_all, 2, peer_of(i), peer_of(i)).wait_recv())

    mixed = mixed_all[...].astype(jnp.float32)
    scale = lax.rsqrt(jnp.mean(mixed * mixed, axis=-1, keepdims=True) + 1e-05)
    gains = gain[...].astype(jnp.float32)
    gain_row = jnp.concatenate([gains[i : i + 1] for i in range(gains.shape[0])], axis=1)
    normed = (mixed * scale * gain_row).astype(jnp.bfloat16)
    normed_ref[...] = normed
    normed = normed.astype(jnp.float32)
    router_rows = router[...].astype(jnp.float32)
    logits = [
        jnp.sum(normed * router_rows[e : e + 1], axis=-1, keepdims=True) for e in range(EXPERTS)
    ]
    row = lax.broadcasted_iota(jnp.int32, (slots, 1), 0)
    chosen = []
    for k in range(2):
        ids = jnp.zeros_like(row)
        for s in range(slots):
            ids = jnp.where(row == s, expert_ids[k, s], ids)
        chosen.append(ids)
    picked = [
        sum(jnp.where(chosen[k] == e, logits[e], 0.0) for e in range(EXPERTS)) for k in range(2)
    ]
    expert_now = (me * units) // FF
    share = jnp.where(chosen[0] == expert_now, jax.nn.sigmoid(picked[0] - picked[1]), 0.0)
    share += jnp.where(chosen[1] == expert_now, jax.nn.sigmoid(picked[1] - picked[0]), 0.0)

    gate_acc[...] = jnp.zeros_like(gate_acc)
    up_acc[...] = jnp.zeros_like(up_acc)

    def gu_step(k):
        gu_copy(k).wait()
        rows = pl.ds(pl.multiple_of(k * depth, depth), depth)
        piece = normed_ref[:, rows]
        gate_acc[...] += jnp.dot(piece, gate_up[0, rows, :], preferred_element_type=jnp.float32)
        up_acc[...] += jnp.dot(piece, gate_up[1, rows, :], preferred_element_type=jnp.float32)

    each(GU_CHUNKS, gu_step)
    gate = gate_acc[...]
    act = (gate * jax.nn.sigmoid(gate) * up_acc[...]).astype(jnp.bfloat16)

    def term_of(c):
        down_copy(c).wait()
        return share * jnp.dot(act, down[:, columns(c)], preferred_element_type=jnp.float32)

    def term_step(i):
        c = peer_of(i)
        term_send[c] = term_of(c).astype(jnp.bfloat16)
        term_copy(c, me).start()

    each(n - 1, term_step)
    total = local_mixed.astype(jnp.float32) + term_of(me)
    term_recv[me] = jnp.zeros((slots, width), jnp.bfloat16)
    every(n - 1, lambda i: term_copy(peer_of(i), peer_of(i)).wait_recv())
    for i in range(n):
        total += term_recv[i].astype(jnp.float32)
    out_ref[...] = total.astype(jnp.bfloat16)

    def drain(i):
        c = peer_of(i)
        part_copy(c, me).wait_send()
        share_copy(attn_all, 1, c, me).wait_send()
        share_copy(mixed_all, 2, c, me).wait_send()
        term_copy(c, me).wait_send()

    every(n - 1, drain)


def fused_layer(
    n,
    hidden,
    queries,
    cache_kv,
    cache_len,
    inserted_key_value,
    insert_slot,
    prefix_len,
    out_weight,
    norm_gain,
    router_weight,
    expert_ids,
    gate_up,
    down_proj,
):
    slots, features = queries.shape
    entries = slots + insert_slot.shape[0]
    width = out_weight.shape[1]
    units = gate_up.shape[2]
    any_space = pl.BlockSpec(memory_space=pl.ANY)
    smem = pl.BlockSpec(memory_space=pltpu.SMEM)
    bf16, f32 = jnp.bfloat16, jnp.float32
    return pl.pallas_call(
        functools.partial(fused_kernel, n),
        out_shape=jax.ShapeDtypeStruct((slots, width), bf16),
        in_specs=[smem] * 4 + [any_space] * 9,
        out_specs=pl.BlockSpec(memory_space=pltpu.VMEM),
        scratch_shapes=[
            pltpu.VMEM((slots, width), bf16),
            pltpu.VMEM((slots, features), bf16),
            pltpu.VMEM((2, entries) + cache_kv.shape[2:], bf16),
            pltpu.VMEM(out_weight.shape, bf16),
            pltpu.VMEM((features // HEAD_SIZE, HEAD_SIZE), bf16),
            pltpu.VMEM((EXPERTS, features), bf16),
            pltpu.VMEM(gate_up.shape, bf16),
            pltpu.VMEM(down_proj.shape, bf16),
            pltpu.VMEM((n, 3 * slots, HEAD_SIZE), bf16),
            pltpu.VMEM((n, 3 * slots, HEAD_SIZE), bf16),
            pltpu.VMEM((slots, features), bf16),
            pltpu.VMEM((slots, features), bf16),
            pltpu.VMEM((slots, features), bf16),
            pltpu.VMEM((slots, units), f32),
            pltpu.VMEM((slots, units), f32),
            pltpu.VMEM((n, slots, width), bf16),
            pltpu.VMEM((n, slots, width), bf16),
            pltpu.SemaphoreType.DMA((7,)),
            pltpu.SemaphoreType.DMA((GU_CHUNKS,)),
            pltpu.SemaphoreType.DMA((n,)),
            pltpu.SemaphoreType.DMA((4, n)),
            pltpu.SemaphoreType.DMA((4, n)),
        ],
        compiler_params=pltpu.CompilerParams(
            collective_id=0, has_side_effects=True, vmem_limit_bytes=60 * 1024 * 1024
        ),
        name="layer",
    )(
        cache_len,
        insert_slot,
        prefix_len,
        expert_ids.T,
        hidden,
        queries,
        cache_kv,
        inserted_key_value,
        out_weight,
        norm_gain.reshape(-1, HEAD_SIZE),
        router_weight.T,
        gate_up,
        down_proj,
    )


def on_device(*args):
    n = lax.axis_size("blk")
    queries, cache_kv, out_weight, gate_up = args[1], args[2], args[7], args[11]
    ctx, slots = cache_kv.shape[2], queries.shape[0]
    fits = (
        QUERY_HEADS == 2 * n
        and out_weight.shape[1] == 2 * HEAD_SIZE
        and ctx % 16 == 0
        and ctx & (ctx - 1) == 0
        and slots % 16 == 0
        and slots & (slots - 1) == 0
        and gate_up.shape[1] % (128 * GU_CHUNKS) == 0
        and gate_up.shape[2] % 128 == 0
        and FF % gate_up.shape[2] == 0
    )
    return fused_layer(n, *args) if fits else plain_layer(*args)


def solution(mesh):
    in_specs = (
        P("rep", "blk"),
        P("rep", None),
        P(None, "rep", "blk", None),
        P("rep"),
        P(None, "rep", "blk", None),
        P("rep"),
        P("rep"),
        P(None, "blk"),
        P(),
        P(),
        P("rep", None),
        P(None, None, "blk"),
        P("blk", None),
    )
    out_specs = P("rep", "blk")
    return jax.shard_map(
        on_device, mesh=mesh, in_specs=in_specs, out_specs=out_specs, check_vma=False
    )
```
